32 devices in a mesh: blk: 8 (over z, x), ga: 4 (over y, core).
Axes of the slice: x: 2, y: 2, z: 4, core: 2. Of those that a mesh axis runs over, the one named last changes fastest.
Arguments:
- pair_val: bfloat16 [16, 16, 16, 2048], P('blk', None, None, 'ga'), may hold values from -0.125 to 0.125
- pair_con: bfloat16 [16, 16, 16, 2048], P('blk', None, None, 'ga'), may hold values from -6 to 6
- screened: bfloat16 [16, 2048, 2048], P('blk', None, 'ga'), may hold values from -0.125 to 0.125
- amplitude: bfloat16 [16, 16], P('blk'), may hold values from -6 to 6
- qmap: int32 [16, 16], P('blk'), may hold values from 0 to 15, as said below
Outputs:
- kernel_x: float32 [16, 16], P('blk')
The draws below stay inside these ranges and needn't reach their ends.
Inputs may be any that keep to these rules, and one draw needn't show every extreme that they name: qmap[k, k'] is the label of the difference k - k' (periodic) on a grid of 8 by 2 points, with the points and the differences labelled at random; every row and every column holds each label once.
All inputs are finite; a program needn't handle non-finite values.
Results may differ from the reference program's by a relative error of at most 0.004.
Values may be sent and summed in bfloat16 or wider, within the bound.
A program may use at most 64 MiB of HBM per device.

```python
import jax
import jax.numpy as jnp
from jax import lax

NV = 4
NC = 4
NG = 2048
GRID_X = 8
NK = 16


def draw_qmap(key, part):
    point_order = jax.random.permutation(jax.random.fold_in(key, 11), NK)
    label_order = jax.random.permutation(jax.random.fold_in(key, 23), NK)
    rows_y = NK // GRID_X
    coord_x = point_order % GRID_X
    coord_y = point_order // GRID_X
    diff_x = (coord_x[:, None] - coord_x[None, :]) % GRID_X
    diff_y = (coord_y[:, None] - coord_y[None, :]) % rows_y
    return label_order[diff_y * GRID_X + diff_x].astype(jnp.int32)


def block_scale(own_key, shape, shards, smallest, high):
    factor_of, own = 1.0, jax.random.fold_in(own_key, 6)
    for dim, shards_of in shards:
        steps = jnp.exp(jax.random.uniform(jax.random.fold_in(own, dim), (shards_of,), jnp.float32, smallest / len(shards), high / len(shards)))
        factor_of = factor_of * jnp.repeat(steps, shape[dim] // shards_of).reshape([-1 if axis == dim else 1 for axis in range(len(shape))])
    return factor_of


def bell_draw(stream_key, shape, width, reach, pieces=(), held_as=jnp.bfloat16):
    values = width * jax.random.normal(stream_key, shape, jnp.float32)
    if pieces:
        values = values * block_scale(stream_key, shape, pieces, -0.22, 0.18)
    return jnp.clip(values, -reach, reach).astype(held_as)


def setup_inputs(seed: int = 0) -> dict:
    key_list = jax.random.split(jax.random.key(seed), 6)
    return {
        "pair_val": bell_draw(key_list[0], (NK, NK, NV * NV, NG), NG ** -0.5, 0.125, ((0, 8), (3, 4))),
        "pair_con": bell_draw(key_list[1], (NK, NK, NC * NC, NG), 1.0, 6.0, ((0, 8), (3, 4))),
        "screened": bell_draw(key_list[2], (NK, NG, NG), NG ** -0.5, 0.125, ((0, 8), (2, 4))),
        "amplitude": bell_draw(key_list[3], (NK, NV * NC), 1.0, 6.0, ((0, 8),)),
        "qmap": draw_qmap(jax.random.fold_in(key_list[5], 71), 0),
    }


def inverse_rows(qmap):
    total = qmap.shape[1]
    labels = jnp.arange(total, dtype=jnp.int32)
    hits = (qmap[:, :, None] == labels[None, None, :]).astype(jnp.int32)
    return jnp.sum(hits * labels[None, :, None], axis=1).astype(jnp.int32)


def reference(pair_val, pair_con, screened, amplitude, qmap):
    total = qmap.shape[0]
    partner = inverse_rows(qmap)
    rows = jnp.arange(total, dtype=jnp.int32)

    def per_label(label):
        chosen = lax.dynamic_index_in_dim(partner, label, 1, keepdims=False).astype(jnp.int32)
        values = pair_val[rows, chosen].astype(jnp.float32).reshape(total, NV, NV, NG)
        cons = pair_con[rows, chosen]
        amps = amplitude[chosen].astype(jnp.float32).reshape(total, NV, NC)
        zeta = jnp.einsum('navg,nvc->nacg', values, amps).astype(jnp.bfloat16)
        zeta = lax.optimization_barrier(zeta).astype(jnp.float32)
        weights = lax.dynamic_index_in_dim(screened, label, 0, keepdims=False)
        unit = jnp.dot(cons.reshape(total * NC * NC, NG), weights, preferred_element_type=jnp.float32).astype(jnp.bfloat16)
        unit = lax.optimization_barrier(unit).astype(jnp.float32).reshape(total, NC, NC, NG)
        return jnp.einsum('ncyg,nayg->nac', unit, zeta).reshape(total, NV * NC)

    parts = lax.map(per_label, rows)
    return jnp.sum(parts, 0) / total
```

```python
import functools

import jax
import jax.numpy as jnp
from jax import lax
from jax.experimental import pallas as pl
from jax.experimental.pallas import tpu as pltpu
from jax.sharding import PartitionSpec as P

NV = 4
NC = 4
ROWS = 16
TILE = 256
MESH = pl.DeviceIdType.MESH
F32 = jnp.float32
BF16 = jnp.bfloat16


def iota(shape, dim):
    return lax.broadcasted_iota(jnp.int32, shape, dim)


def one_hot(mask):
    return jnp.where(mask, 1.0, 0.0).astype(F32)


def kernel(
    blks, gas, val_hbm, con_hbm, w_hbm, amp_ref, q_ref, out_ref,
    val_in, con_in, w_in, con_send, zeta_send, con_all, zeta_all, amp_all, amp_rows, unit, contrib, fin,
    load_sem, amp_ssem, amp_rsem, con_ssem, con_rsem, zeta_ssem, zeta_rsem,
    row_ssem, row_rsem, core_ssem, core_rsem, fin_ssem, fin_rsem,
):
    me, ga = lax.axis_index("blk"), lax.axis_index("ga")
    local_k, total = q_ref.shape
    labels, width = w_in.shape[0], w_in.shape[2]
    wide = total * ROWS
    lane = me * gas + ga
    devices = blks * gas
    rings = gas // 2
    other = ga + 1 - 2 * (ga % 2)

    loads = [
        pltpu.make_async_copy(con_hbm, con_in, load_sem.at[0]),
        pltpu.make_async_copy(val_hbm, val_in, load_sem.at[1]),
        pltpu.make_async_copy(w_hbm, w_in, load_sem.at[2]),
    ]
    for load in loads:
        load.start()

    barrier = pltpu.get_barrier_semaphore()

    def greet(i, carry):
        to = (lane + i) % devices
        pl.semaphore_signal(barrier, inc=1, device_id=(to // gas, to % gas), device_id_type=MESH)
        return carry

    lax.fori_loop(1, devices, greet, 0)

    def amp_copy(step):
        return pltpu.make_async_remote_copy(
            src_ref=amp_ref, dst_ref=amp_all.at[me],
            send_sem=amp_ssem.at[step], recv_sem=amp_rsem.at[step],
            device_id=((me + step) % blks, ga), device_id_type=MESH)

    def con_copy(step):
        to = (me + step) % blks
        return pltpu.make_async_remote_copy(
            src_ref=con_send.at[to], dst_ref=con_all.at[ga, me],
            send_sem=con_ssem.at[step], recv_sem=con_rsem.at[step],
            device_id=(to, ga), device_id_type=MESH)

    def zeta_copy(step):
        to = (me + step) % blks
        return pltpu.make_async_remote_copy(
            src_ref=zeta_send.at[to], dst_ref=zeta_all.at[me],
            send_sem=zeta_ssem.at[step], recv_sem=zeta_rsem.at[step],
            device_id=(to, ga), device_id_type=MESH)

    def row_copy(hop, step):
        owner = (me + blks - step) % blks
        return pltpu.make_async_remote_copy(
            src_ref=con_all.at[ga, owner], dst_ref=con_all.at[ga, owner],
            send_sem=row_ssem.at[hop, step], recv_sem=row_rsem.at[hop, step],
            device_id=(me, (ga + 2 * hop) % gas), device_id_type=MESH)

    def core_copy(hop, step):
        owner = (me + blks - step) % blks
        part = (ga + gas - 2 * hop) % gas
        return pltpu.make_async_remote_copy(
            src_ref=con_all.at[part, owner], dst_ref=con_all.at[part, owner],
            send_sem=core_ssem.at[hop, step], recv_sem=core_rsem.at[hop, step],
            device_id=(me, other), device_id_type=MESH)

    def order(i):
        return (blks // 2 + i - 1) % (blks - 1) + 1

    def each_step(action):
        def run(i, carry):
            action(order(i))
            return carry

        lax.fori_loop(0, blks - 1, run, 0)

    spread = one_hot(iota((total, wide), 1) >> 4 == iota((total, wide), 0)).astype(BF16)
    labels_at = jnp.dot(q_ref[...].astype(F32).astype(BF16), spread, preferred_element_type=F32).astype(jnp.int32)
    row, col = iota((TILE, wide), 0), iota((TILE, wide), 1)
    same_pair = (row & 15) == (col & 15)
    same_band = ((row >> 2) & 3) == ((col >> 2) & 3)
    chunk_labels = TILE // ROWS
    chunk_blks = chunk_labels // labels

    def stored(ref, k, chunk, value):
        blocks = value.astype(BF16).reshape(chunk_blks, labels, ROWS, width)
        ref[pl.ds(chunk * chunk_blks, chunk_blks), :, pl.ds(k * ROWS, ROWS), :] = blocks

    hits = {}
    for k in range(local_k):
        for chunk in range(wide // TILE):
            hits[k, chunk] = labels_at[k : k + 1, :] == (row >> 4) + chunk * chunk_labels
    loads[0].wait()
    for k in range(local_k):
        con_k = con_in[k].reshape(wide, width)
        for chunk in range(wide // TILE):
            pick = one_hot(hits[k, chunk] & same_pair).astype(BF16)
            stored(con_send, k, chunk, jnp.dot(pick, con_k, preferred_element_type=F32))
    con_all[ga, me] = con_send[me]
    amp_all[me] = amp_ref[...]

    pl.semaphore_wait(barrier, devices - 1)
    each_step(lambda step: amp_copy(step).start())
    each_step(lambda step: con_copy(step).start())
    for hop in range(1, rings):
        row_copy(hop, 0).start()
    core_copy(0, 0).start()

    each_step(lambda step: amp_copy(step).wait_recv())
    for blk in range(blks):
        amp_rows[pl.ds(blk * local_k, local_k), :] = amp_all[blk].astype(F32)
    amps = lax.dot_general(
        amp_rows[...].astype(BF16), spread, (((0,), (0,)), ((), ())), preferred_element_type=F32)
    pair, at = iota((NV * NC, wide), 0), iota((NV * NC, wide), 1)
    amps = jnp.where((pair >> 2) == (at & 3), amps, 0.0).astype(BF16)
    lines, pairs = iota((TILE, NV * NC), 0), iota((TILE, NV * NC), 1)
    amps = jnp.dot(one_hot((lines & 3) == (pairs & 3)).astype(BF16), amps, preferred_element_type=F32)
    amps = jnp.where(same_band, amps, 0.0)
    loads[1].wait()
    for k in range(local_k):
        val_k = val_in[k].reshape(wide, width)
        for chunk in range(wide // TILE):
            mix = jnp.where(hits[k, chunk], amps, 0.0).astype(BF16)
            stored(zeta_send, k, chunk, jnp.dot(mix, val_k, preferred_element_type=F32))
    zeta_all[me] = zeta_send[me]
    each_step(lambda step: zeta_copy(step).start())

    def relay(i, carry):
        step = order(i)
        con_copy(step).wait_recv()
        for hop in range(1, rings):
            row_copy(hop, step).start()
        core_copy(0, step).start()
        before = jnp.where(i == 0, 0, order(jnp.maximum(i - 1, 0)))
        for hop in range(1, rings):
            row_copy(hop, before).wait_recv()
            core_copy(hop, before).start()
        return carry

    lax.fori_loop(0, blks - 1, relay, 0)
    last = (blks // 2 + blks - 3) % (blks - 1) + 1
    for hop in range(1, rings):
        row_copy(hop, last).wait_recv()
        core_copy(hop, last).start()

    def gathered(step, carry):
        for hop in range(rings):
            core_copy(hop, step).wait_recv()
        return carry

    loads[2].wait()
    lax.fori_loop(0, blks, gathered, 0)

    group = TILE // (local_k * ROWS)
    for part in range(blks // group):
        for label in range(labels):
            summed = None
            for quarter in range(gas):
                cons = con_all[quarter, pl.ds(part * group, group), label].reshape(TILE, width)
                term = jnp.dot(cons, w_in[label, pl.ds(quarter * width, width), :], preferred_element_type=F32)
                summed = term if summed is None else summed + term
            unit[label, pl.ds(part * TILE, TILE), :] = summed.astype(BF16)

    each_step(lambda step: zeta_copy(step).wait_recv())

    r, s = iota((TILE, TILE), 0), iota((TILE, TILE), 1)
    kept = ((r >> 4) == (s >> 4)) & ((r & 3) == (s & 3))
    c_at, w_of = iota((ROWS, 128), 0), iota((ROWS, 128), 1)
    by_c = one_hot(((c_at >> 2) == (w_of & 3)) & (w_of < ROWS))
    s_at, w_at = iota((TILE, 128), 0), iota((TILE, 128), 1)
    by_v = ((s_at >> 2) & 3) == (w_at >> 2)
    slot, of = iota((group * 8, TILE), 0), iota((group * 8, TILE), 1)
    by_k = one_hot(((slot & 7) < local_k) & ((of >> 4) == (slot >> 3) * local_k + (slot & 7)))
    for part in range(blks // group):
        cross = None
        for label in range(labels):
            zetas = zeta_all[pl.ds(part * group, group), label].reshape(TILE, width)
            term = lax.dot_general(
                unit[label, pl.ds(part * TILE, TILE), :], zetas, (((1,), (1,)), ((), ())),
                preferred_element_type=F32)
            cross = term if cross is None else cross + term
        folded = jnp.sum(jnp.where(kept, cross, 0.0).reshape(TILE // ROWS, ROWS, TILE), axis=0)
        spread_c = lax.dot_general(
            folded, by_c, (((0,), (0,)), ((), ())), precision=lax.Precision.HIGHEST, preferred_element_type=F32)
        spread_c = jnp.where(by_v, spread_c, 0.0)
        per_k = jnp.dot(by_k, spread_c, precision=lax.Precision.HIGHEST, preferred_element_type=F32)
        contrib[pl.ds(part * group, group)] = per_k.reshape(group, 8, 128)

    def fin_copy(i):
        to = (lane + i) % devices
        return pltpu.make_async_remote_copy(
            src_ref=contrib.at[to // gas], dst_ref=fin.at[i],
            send_sem=fin_ssem.at[i], recv_sem=fin_rsem.at[i],
            device_id=(to // gas, to % gas), device_id_type=MESH)

    def every(action):
        def run(i, carry):
            action(fin_copy(i))
            return carry

        lax.fori_loop(1, devices, run, 0)

    every(lambda copy: copy.start())
    fin[0] = contrib[me]

    each_step(lambda step: amp_copy(step).wait_send())
    each_step(lambda step: con_copy(step).wait_send())
    each_step(lambda step: zeta_copy(step).wait_send())

    def relayed(step, carry):
        for hop in range(1, rings):
            row_copy(hop, step).wait_send()
        for hop in range(rings):
            core_copy(hop, step).wait_send()
        return carry

    lax.fori_loop(0, blks, relayed, 0)
    every(lambda copy: copy.wait())
    out_ref[...] = jnp.sum(fin[...], axis=0)[:local_k, :ROWS] / total


def body(pair_val, pair_con, screened, amplitude, qmap, *, blks, gas):
    local_k, total, _, width = pair_val.shape
    labels, depth, _ = screened.shape
    devices = blks * gas
    dma = pltpu.SemaphoreType.DMA
    anywhere = pl.BlockSpec(memory_space=pl.ANY)
    vmem = pl.BlockSpec(memory_space=pltpu.VMEM)
    block = (labels, local_k * ROWS, width)
    return pl.pallas_call(
        functools.partial(kernel, blks, gas),
        out_shape=jax.ShapeDtypeStruct((local_k, NV * NC), F32),
        in_specs=[anywhere, anywhere, anywhere, vmem, vmem],
        out_specs=vmem,
        scratch_shapes=[
            pltpu.VMEM(pair_val.shape, BF16),
            pltpu.VMEM(pair_con.shape, BF16),
            pltpu.VMEM(screened.shape, BF16),
            pltpu.VMEM((blks,) + block, BF16),
            pltpu.VMEM((blks,) + block, BF16),
            pltpu.VMEM((gas, blks) + block, BF16),
            pltpu.VMEM((blks,) + block, BF16),
            pltpu.VMEM((blks,) + amplitude.shape, BF16),
            pltpu.VMEM((total, NV * NC), F32),
            pltpu.VMEM((labels, total * ROWS, width), BF16),
            pltpu.VMEM((blks, 8, 128), F32),
            pltpu.VMEM((devices, 8, 128), F32),
            dma((3,)),
            dma((blks,)), dma((blks,)), dma((blks,)), dma((blks,)), dma((blks,)), dma((blks,)),
            dma((gas // 2, blks)), dma((gas // 2, blks)), dma((gas // 2, blks)), dma((gas // 2, blks)),
            dma((devices,)), dma((devices,)),
        ],
        compiler_params=pltpu.CompilerParams(
            collective_id=0, has_side_effects=True, vmem_limit_bytes=60 * 1024 * 1024),
    )(pair_val, pair_con, screened, amplitude, qmap)


def solution(mesh):
    placed = (
        P("blk", None, None, "ga"),
        P("blk", None, None, "ga"),
        P("blk", None, "ga"),
        P("blk", None),
        P("blk", None),
    )
    sizes = {"blks": mesh.shape["blk"], "gas": mesh.shape["ga"]}
    return jax.shard_map(
        functools.partial(body, **sizes), mesh=mesh, in_specs=placed, out_specs=P("blk", None), check_vma=False
    )
```

```python
import functools

import jax
import jax.numpy as jnp
from jax import lax
from jax.experimental import pallas as pl
from jax.experimental.pallas import tpu as pltpu
from jax.sharding import PartitionSpec as P

NV = 4
NC = 4
ROWS = 16
TILE = 256
MESH = pl.DeviceIdType.MESH
F32 = jnp.float32
BF16 = jnp.bfloat16


def iota(shape, dim):
    return lax.broadcasted_iota(jnp.int32, shape, dim)


def one_hot(mask):
    return jnp.where(mask, 1.0, 0.0).astype(F32)


def kernel(
    blks, gas, val_hbm, con_hbm, w_hbm, amp_ref, q_ref, out_ref,
    val_in, con_in, w_in, con_send, zeta_send, con_all, zeta_all, amp_all, amp_rows, unit, contrib, fin,
    load_sem, amp_ssem, amp_rsem, con_ssem, con_rsem, zeta_ssem, zeta_rsem,
    row_ssem, row_rsem, core_ssem, core_rsem, fin_ssem, fin_rsem, hop_sem,
):
    me, ga = lax.axis_index("blk"), lax.axis_index("ga")
    local_k, total = q_ref.shape
    labels, width = w_in.shape[0], w_in.shape[2]
    wide = total * ROWS
    lane = me * gas + ga
    devices = blks * gas
    rings = gas // 2
    other = ga + 1 - 2 * (ga % 2)

    loads = [
        pltpu.make_async_copy(con_hbm, con_in, load_sem.at[0]),
        pltpu.make_async_copy(val_hbm, val_in, load_sem.at[1]),
        pltpu.make_async_copy(w_hbm, w_in, load_sem.at[2]),
    ]
    for load in loads:
        load.start()

    line = blks // 2
    z, x = me // 2, me % 2
    shifts = [(0, 1)]
    for far in range(1, line):
        shifts += [(far, 0), (-far, 0), (far, 1), (-far, 1)]
    shifts.sort(key=lambda shift: abs(shift[0]) + shift[1])

    def reach(shift):
        return abs(shift[0]) + shift[1]

    def index_of(shift):
        return (shift[0] + line - 1) * 2 + shift[1]

    def to_blk(shift):
        return (z + shift[0]) * 2 + (x + shift[1]) % 2

    def from_blk(shift):
        return (z - shift[0]) * 2 + (x + shift[1]) % 2

    def sent(chosen, action):
        for shift in chosen:
            pl.when((z + shift[0] >= 0) & (z + shift[0] < line))(functools.partial(action, shift))

    def received(chosen, action):
        for shift in chosen:
            pl.when((z - shift[0] >= 0) & (z - shift[0] < line))(functools.partial(action, shift))

    beside = jnp.minimum(z, 1) + jnp.minimum(line - 1 - z, 1)
    barrier = pltpu.get_barrier_semaphore()

    def greet(semaphore):
        for far in (1, -1):
            @pl.when((z + far >= 0) & (z + far < line))
            def _():
                pl.semaphore_signal(semaphore, inc=1, device_id=(me + 2 * far, ga), device_id_type=MESH)

    greet(barrier)
    pl.semaphore_signal(barrier, inc=1, device_id=(z * 2 + (x + 1) % 2, ga), device_id_type=MESH)
    pl.semaphore_signal(barrier, inc=1, device_id=(me, other), device_id_type=MESH)
    for hop in range(1, rings):
        pl.semaphore_signal(barrier, inc=1, device_id=(me, (ga + 2 * hop) % gas), device_id_type=MESH)

    def amp_copy(shift):
        at = index_of(shift)
        return pltpu.make_async_remote_copy(
            src_ref=amp_ref, dst_ref=amp_all.at[me],
            send_sem=amp_ssem.at[at], recv_sem=amp_rsem.at[at],
            device_id=(to_blk(shift), ga), device_id_type=MESH)

    def con_copy(shift):
        at = index_of(shift)
        return pltpu.make_async_remote_copy(
            src_ref=con_send.at[to_blk(shift)], dst_ref=con_all.at[ga, me],
            send_sem=con_ssem.at[at], recv_sem=con_rsem.at[at],
            device_id=(to_blk(shift), ga), device_id_type=MESH)

    def zeta_copy(shift):
        at = index_of(shift)
        return pltpu.make_async_remote_copy(
            src_ref=zeta_send.at[to_blk(shift)], dst_ref=zeta_all.at[me],
            send_sem=zeta_ssem.at[at], recv_sem=zeta_rsem.at[at],
            device_id=(to_blk(shift), ga), device_id_type=MESH)

    def arrival(ref, semaphores, shift):
        at = index_of(shift)
        return pltpu.make_async_remote_copy(
            src_ref=ref, dst_ref=ref, send_sem=con_ssem.at[at], recv_sem=semaphores.at[at],
            device_id=(from_blk(shift), ga), device_id_type=MESH)

    def amp_arrival(shift):
        return arrival(amp_all.at[from_blk(shift)], amp_rsem, shift)

    def con_arrival(shift):
        return arrival(con_all.at[ga, from_blk(shift)], con_rsem, shift)

    def zeta_arrival(shift):
        return arrival(zeta_all.at[from_blk(shift)], zeta_rsem, shift)

    def row_copy(hop, owner, at):
        return pltpu.make_async_remote_copy(
            src_ref=con_all.at[ga, owner], dst_ref=con_all.at[ga, owner],
            send_sem=row_ssem.at[hop, at], recv_sem=row_rsem.at[hop, at],
            device_id=(me, (ga + 2 * hop) % gas), device_id_type=MESH)

    def core_copy(hop, owner, at):
        part = (ga + gas - 2 * hop) % gas
        return pltpu.make_async_remote_copy(
            src_ref=con_all.at[part, owner], dst_ref=con_all.at[part, owner],
            send_sem=core_ssem.at[hop, at], recv_sem=core_rsem.at[hop, at],
            device_id=(me, other), device_id_type=MESH)

    def hand_on(owner, at):
        for hop in range(1, rings):
            row_copy(hop, owner, at).start()
        core_copy(0, owner, at).start()

    def across(owner, at):
        for hop in range(1, rings):
            row_copy(hop, owner, at).wait_recv()
            core_copy(hop, owner, at).start()

    def relay(shift):
        con_arrival(shift).wait_recv()
        hand_on(from_blk(shift), index_of(shift))

    spread = one_hot(iota((total, wide), 1) >> 4 == iota((total, wide), 0)).astype(BF16)
    labels_at = jnp.dot(q_ref[...].astype(F32).astype(BF16), spread, preferred_element_type=F32).astype(jnp.int32)
    row, col = iota((TILE, wide), 0), iota((TILE, wide), 1)
    same_pair = (row & 15) == (col & 15)
    same_band = ((row >> 2) & 3) == ((col >> 2) & 3)
    chunk_labels = TILE // ROWS
    chunk_blks = chunk_labels // labels

    def stored(ref, k, chunk, value):
        blocks = value.astype(BF16).reshape(chunk_blks, labels, ROWS, width)
        ref[pl.ds(chunk * chunk_blks, chunk_blks), :, pl.ds(k * ROWS, ROWS), :] = blocks

    hits = {}
    for k in range(local_k):
        for chunk in range(wide // TILE):
            hits[k, chunk] = labels_at[k : k + 1, :] == (row >> 4) + chunk * chunk_labels
    loads[0].wait()
    for k in range(local_k):
        con_k = con_in[k].reshape(wide, width)
        for chunk in range(wide // TILE):
            pick = one_hot(hits[k, chunk] & same_pair).astype(BF16)
            stored(con_send, k, chunk, jnp.dot(pick, con_k, preferred_element_type=F32))
    con_all[ga, me] = con_send[me]
    amp_all[me] = amp_ref[...]

    pl.semaphore_wait(barrier, beside + rings + 1)
    for phase in range(1, line + 1):
        if phase > 1:
            greet(hop_sem.at[phase])
            pl.semaphore_wait(hop_sem.at[phase], beside)
        near = [shift for shift in shifts if reach(shift) == phase]
        sent(near, lambda shift: amp_copy(shift).start())
        sent(near, lambda shift: con_copy(shift).start())
        if phase == 1:
            hand_on(me, 2 * line - 2)
    near = [shift for shift in shifts if reach(shift) == 1]
    rest = [shift for shift in shifts if reach(shift) > 1]
    received(near, relay)

    received(shifts, lambda shift: amp_arrival(shift).wait_recv())
    for blk in range(blks):
        amp_rows[pl.ds(blk * local_k, local_k), :] = amp_all[blk].astype(F32)
    amps = lax.dot_general(
        amp_rows[...].astype(BF16), spread, (((0,), (0,)), ((), ())), preferred_element_type=F32)
    pair, at = iota((NV * NC, wide), 0), iota((NV * NC, wide), 1)
    amps = jnp.where((pair >> 2) == (at & 3), amps, 0.0).astype(BF16)
    lines, pairs = iota((TILE, NV * NC), 0), iota((TILE, NV * NC), 1)
    amps = jnp.dot(one_hot((lines & 3) == (pairs & 3)).astype(BF16), amps, preferred_element_type=F32)
    amps = jnp.where(same_band, amps, 0.0)
    loads[1].wait()
    for k in range(local_k):
        val_k = val_in[k].reshape(wide, width)
        for chunk in range(wide // TILE):
            mix = jnp.where(hits[k, chunk], amps, 0.0).astype(BF16)
            stored(zeta_send, k, chunk, jnp.dot(mix, val_k, preferred_element_type=F32))
    zeta_all[me] = zeta_send[me]
    sent(shifts[::-1], lambda shift: zeta_copy(shift).start())

    received(rest, relay)
    across(me, 2 * line - 2)
    received(shifts, lambda shift: across(from_blk(shift), index_of(shift)))

    def gathered(owner, at):
        for hop in range(rings):
            core_copy(hop, owner, at).wait_recv()

    loads[2].wait()
    gathered(me, 2 * line - 2)
    received(shifts, lambda shift: gathered(from_blk(shift), index_of(shift)))

    group = TILE // (local_k * ROWS)
    for part in range(blks // group):
        for label in range(labels):
            summed = None
            for quarter in range(gas):
                cons = con_all[quarter, pl.ds(part * group, group), label].reshape(TILE, width)
                term = jnp.dot(cons, w_in[label, pl.ds(quarter * width, width), :], preferred_element_type=F32)
                summed = term if summed is None else summed + term
            unit[label, pl.ds(part * TILE, TILE), :] = summed.astype(BF16)

    received(shifts, lambda shift: zeta_arrival(shift).wait_recv())

    r, s = iota((TILE, TILE), 0), iota((TILE, TILE), 1)
    kept = ((r >> 4) == (s >> 4)) & ((r & 3) == (s & 3))
    c_at, w_of = iota((ROWS, 128), 0), iota((ROWS, 128), 1)
    by_c = one_hot((c_at >> 2) == (w_of & 3))
    s_at, w_at = iota((TILE, 128), 0), iota((TILE, 128), 1)
    by_v = (((s_at >> 2) & 3) == ((w_at >> 2) & 3)) & ((s_at >> 4) % local_k == (w_at >> 4))
    for part in range(blks // group):
        cross = None
        for label in range(labels):
            zetas = zeta_all[pl.ds(part * group, group), label].reshape(TILE, width)
            term = lax.dot_general(
                unit[label, pl.ds(part * TILE, TILE), :], zetas, (((1,), (1,)), ((), ())),
                preferred_element_type=F32)
            cross = term if cross is None else cross + term
        folded = jnp.sum(jnp.where(kept, cross, 0.0).reshape(TILE // ROWS, ROWS, TILE), axis=0)
        spread_c = lax.dot_general(
            folded, by_c, (((0,), (0,)), ((), ())), precision=lax.Precision.HIGHEST, preferred_element_type=F32)
        spread_c = jnp.where(by_v, spread_c, 0.0)
        per_k = jnp.sum(spread_c.reshape(group, TILE // group, 128), axis=1)
        for at in range(group):
            contrib[part * group + at] = per_k[at : at + 1]

    def fin_copy(i):
        to = (lane + i) % devices
        return pltpu.make_async_remote_copy(
            src_ref=contrib.at[to // gas], dst_ref=fin.at[i],
            send_sem=fin_ssem.at[i], recv_sem=fin_rsem.at[i],
            device_id=(to // gas, to % gas), device_id_type=MESH)

    def every(action):
        def run(i, carry):
            action(fin_copy(i))
            return carry

        lax.fori_loop(1, devices, run, 0)

    every(lambda copy: copy.start())
    fin[0] = contrib[me]

    sent(shifts, lambda shift: amp_copy(shift).wait_send())
    sent(shifts, lambda shift: con_copy(shift).wait_send())
    sent(shifts, lambda shift: zeta_copy(shift).wait_send())

    def relayed(owner, at):
        for hop in range(1, rings):
            row_copy(hop, owner, at).wait_send()
        for hop in range(rings):
            core_copy(hop, owner, at).wait_send()

    relayed(me, 2 * line - 2)
    received(shifts, lambda shift: relayed(from_blk(shift), index_of(shift)))
    every(lambda copy: copy.wait())
    total_row = jnp.sum(fin[...], axis=0) / total
    for k in range(local_k):
        out_ref[k : k + 1, :] = total_row[:, k * ROWS : (k + 1) * ROWS]


def body(pair_val, pair_con, screened, amplitude, qmap, *, blks, gas):
    local_k, total, _, width = pair_val.shape
    labels, depth, _ = screened.shape
    devices = blks * gas
    dma = pltpu.SemaphoreType.DMA
    anywhere = pl.BlockSpec(memory_space=pl.ANY)
    vmem = pl.BlockSpec(memory_space=pltpu.VMEM)
    block = (labels, local_k * ROWS, width)
    return pl.pallas_call(
        functools.partial(kernel, blks, gas),
        out_shape=jax.ShapeDtypeStruct((local_k, NV * NC), F32),
        in_specs=[anywhere, anywhere, anywhere, vmem, vmem],
        out_specs=vmem,
        scratch_shapes=[
            pltpu.VMEM(pair_val.shape, BF16),
            pltpu.VMEM(pair_con.shape, BF16),
            pltpu.VMEM(screened.shape, BF16),
            pltpu.VMEM((blks,) + block, BF16),
            pltpu.VMEM((blks,) + block, BF16),
            pltpu.VMEM((gas, blks) + block, BF16),
            pltpu.VMEM((blks,) + block, BF16),
            pltpu.VMEM((blks,) + amplitude.shape, BF16),
            pltpu.VMEM((total, NV * NC), F32),
            pltpu.VMEM((labels, total * ROWS, width), BF16),
            pltpu.VMEM((blks, 1, 128), F32),
            pltpu.VMEM((devices, 1, 128), F32),
            dma((3,)),
            *[dma((2 * blks - 2,))] * 6,
            *[dma((gas // 2, 2 * blks - 2))] * 4,
            dma((devices,)), dma((devices,)),
            pltpu.SemaphoreType.REGULAR((blks // 2 + 1,)),
        ],
        compiler_params=pltpu.CompilerParams(
            collective_id=0, has_side_effects=True, vmem_limit_bytes=60 * 1024 * 1024),
    )(pair_val, pair_con, screened, amplitude, qmap)


def solution(mesh):
    placed = (
        P("blk", None, None, "ga"),
        P("blk", None, None, "ga"),
        P("blk", None, "ga"),
        P("blk", None),
        P("blk", None),
    )
    sizes = {"blks": mesh.shape["blk"], "gas": mesh.shape["ga"]}
    return jax.shard_map(
        functools.partial(body, **sizes), mesh=mesh, in_specs=placed, out_specs=P("blk", None), check_vma=False
    )
```
